32 devices in a mesh: north: 8 (over z, x), deep: 4 (over y, core).
Axes of the slice: x: 2, y: 2, z: 4, core: 2. Of those that a mesh axis runs over, the one named last changes fastest.
Arguments:
- source: float32 [128, 128, 2048], P(None, 'north', 'deep'), may hold values from -6 to 6
- symbol_x: float32 [128], replicated, may hold values from 0.3 to 3
- symbol_y: float32 [128], replicated, may hold values from 0.3 to 3
- symbol_z: float32 [2048], replicated, may hold values from 0.3 to 3
Outputs:
- coefficients: float32 [64, 64, 1024], P('north', 'deep')
The draws below stay inside these ranges and needn't reach their ends.
All inputs are finite; a program needn't handle non-finite values.
Results may differ from the reference program's by a relative error of at most 0.000071.
Values sent between devices are 32-bit elements; how exact they have to be, the bound alone decides.
A program may use at most 128 MiB of HBM per device.

```python
import jax
import jax.numpy as jnp
from jax import lax

GRID_X = 128
GRID_Y = 128
GRID_Z = 2048


def block_levels(stream_key, shape, shards, least, largest):
    gain = 1.0
    for dim, parts in shards:
        heights = jax.random.uniform(jax.random.fold_in(jax.random.fold_in(stream_key, 6), dim), (parts,), jnp.float32, least / len(shards), largest / len(shards))
        gain = gain * jnp.repeat(jnp.exp(heights), shape[dim] // parts).reshape((-1,) + (1,) * (len(shape) - 1 - dim))
    return gain


def noise(rng, shape, scale, most, shards=(), dtype=jnp.bfloat16):
    level = block_levels(rng, shape, shards, -0.22, 0.18) if shards else 1.0
    entries = jax.random.normal(rng, shape, jnp.float32) * scale * level
    return jnp.minimum(jnp.maximum(entries, -most), most).astype(dtype)


def setup_inputs(seed: int = 0) -> dict:
    arg_keys = jax.random.split(jax.random.key(seed), 5)
    source = noise(arg_keys[0], (GRID_X, GRID_Y, GRID_Z), 1.0, 6.0, ((1, 8), (2, 4)), jnp.float32)
    symbol_x = jnp.clip(jax.random.uniform(arg_keys[1], (GRID_X,), jnp.float32, 0.3, 3.0), 0.3, 3.0)
    symbol_y = jnp.clip(jax.random.uniform(arg_keys[2], (GRID_Y,), jnp.float32, 0.3, 3.0), 0.3, 3.0)
    symbol_z = jnp.clip(jax.random.uniform(arg_keys[3], (GRID_Z,), jnp.float32, 0.3, 3.0), 0.3, 3.0)
    return {"source": source, "symbol_x": symbol_x, "symbol_y": symbol_y, "symbol_z": symbol_z}


def basis_table(count):
    rank = jnp.arange(count)
    angle = jnp.pi / (count + 1) * ((rank[:, None] + 1) * (rank[None, :] + 1) % (2 * count + 2)).astype(jnp.float32)
    return jnp.sin(angle) * (2.0 / (count + 1)) ** 0.5

def along_dim(values, dim):
    moved = jnp.tensordot(values, basis_table(values.shape[dim]), axes=([dim], [0]), precision=lax.Precision.HIGHEST)
    return jnp.moveaxis(moved, -1, dim)

def reference(source, symbol_x, symbol_y, symbol_z):
    coefficients = source
    coefficients = along_dim(coefficients, 0)
    coefficients = lax.slice_in_dim(coefficients, 0, GRID_X // 2, axis=0)
    coefficients = along_dim(coefficients, 1)
    coefficients = lax.slice_in_dim(coefficients, 0, GRID_Y // 2, axis=1)
    coefficients = along_dim(coefficients, 2)
    coefficients = lax.slice_in_dim(coefficients, 0, GRID_Z // 2, axis=2)
    symbol = symbol_x[:GRID_X // 2][:, None, None] + symbol_y[:GRID_Y // 2][None, :, None] + symbol_z[:GRID_Z // 2][None, None, :]
    coefficients = coefficients * lax.rsqrt(symbol)
    return coefficients
```

```python
import jax
import jax.numpy as jnp
import numpy as np
from jax import lax
from jax.sharding import PartitionSpec as P

HIGH = lax.Precision.HIGH


def small_table(rows, modes, count):
    rank = np.outer(rows, modes) % (2 * count + 2)
    return np.pi / (count + 1) * rank


def kept_table(count):
    angle = small_table(np.arange(1, count + 1), np.arange(1, count // 2 + 1), count)
    return jnp.asarray((np.sin(angle) * (2.0 / (count + 1)) ** 0.5).astype(np.float32))


def long_table(count, fine=32):
    modes = np.arange(1, count // 2 + 1)
    gain = (2.0 / (count + 1)) ** 0.5
    coarse = small_table(np.arange(0, count, fine), modes, count)
    step = small_table(np.arange(1, fine + 1), modes, count)
    f32 = lambda v: jnp.asarray(v.astype(np.float32))
    sin_a, cos_a = f32(np.sin(coarse) * gain), f32(np.cos(coarse) * gain)
    sin_b, cos_b = f32(np.sin(step)), f32(np.cos(step))
    table = sin_a[:, None, :] * cos_b[None] + cos_a[:, None, :] * sin_b[None]
    return table.reshape(count, count // 2)


def on_device(source, symbol_x, symbol_y, symbol_z):
    north, deep = lax.axis_size("north"), lax.axis_size("deep")
    nx, ny_part, nz_part = source.shape
    each = nx // 2 // north // deep
    v = jnp.einsum("xk,xyz->kyz", kept_table(nx), source, precision=HIGH)
    v = v.reshape(north, deep, each, ny_part, nz_part)
    v = lax.all_to_all(v, "deep", split_axis=1, concat_axis=4, tiled=True)
    v = v.reshape(north, each, ny_part, nz_part * deep)
    v = jnp.einsum("neyz,zk->neyk", v, long_table(nz_part * deep), precision=HIGH)
    v = lax.all_to_all(v, "north", split_axis=0, concat_axis=2, tiled=True)
    v = v.reshape(each, ny_part * north, v.shape[-1])
    v = jnp.einsum("eyz,yk->ekz", v, kept_table(ny_part * north), precision=HIGH)
    v = lax.all_to_all(v, "deep", split_axis=1, concat_axis=0, tiled=True)
    part_x = lax.dynamic_slice_in_dim(symbol_x, lax.axis_index("north") * v.shape[0], v.shape[0])
    part_y = lax.dynamic_slice_in_dim(symbol_y, lax.axis_index("deep") * v.shape[1], v.shape[1])
    symbol = part_x[:, None, None] + part_y[None, :, None] + symbol_z[: v.shape[2]][None, None, :]
    return v * lax.rsqrt(symbol)


def solution(mesh):
    in_specs = (P(None, "north", "deep"), P(), P(), P())
    out_specs = P("north", "deep", None)
    return jax.shard_map(
        on_device, mesh=mesh, in_specs=in_specs, out_specs=out_specs, check_vma=False
    )
```

```python
import functools

import jax
import jax.numpy as jnp
import numpy as np
from jax import lax
from jax.experimental import pallas as pl
from jax.experimental.pallas import tpu as pltpu
from jax.sharding import PartitionSpec as P

F32, BF16 = jnp.float32, jnp.bfloat16
FINE = 32
TILE = 256


def angles(rows, modes, count):
    rank = np.outer(rows, modes) % (2 * count + 2)
    return np.pi / (count + 1) * rank


def split_np(table):
    high = table.astype(np.float32).astype(BF16)
    low = (table - high.astype(np.float64)).astype(np.float32).astype(BF16)
    return high, low


def left_table(count):
    gain = (2.0 / (count + 1)) ** 0.5
    table = np.sin(angles(np.arange(1, count // 2 + 1), np.arange(1, count + 1), count)) * gain
    return split_np(table)


def stacked(high, low):
    return jnp.asarray(np.block([[high, high], [low, np.zeros_like(low)]]))


def long_tables(count):
    modes = np.arange(1, count // 2 + 1)
    gain = (2.0 / (count + 1)) ** 0.5
    coarse = angles(np.arange(0, count, FINE), modes, count)
    step = angles(np.arange(1, FINE + 1), modes, count)
    f32 = lambda v: jnp.asarray(v.astype(np.float32))
    return f32(np.sin(coarse) * gain), f32(np.cos(coarse) * gain), f32(np.sin(step)), f32(np.cos(step))


def split(values):
    high = values.astype(BF16)
    return high, (values - high.astype(F32)).astype(BF16)


def dot(a, b):
    return jnp.dot(a, b, preferred_element_type=F32)


def kernel(
    north, deep, each,
    src, tx, ty, sin_a, cos_a, sin_b, cos_b,
    out,
    send1, recv1, send2, recv2, send3, recv3, t_high, t_low, left, acc,
    s1, r1, s2, r2, s3, r3,
):
    me_n, me_d = lax.axis_index("north"), lax.axis_index("deep")
    ny_part, nx, nz_part = src.shape
    kept_x = nx // 2
    kept_z = t_high.shape[1]
    rows = ny_part * north

    barrier = pltpu.get_barrier_semaphore()
    for r in range(1, deep):
        pl.semaphore_signal(barrier, inc=1, device_id={"deep": lax.rem(me_d + r, deep)})
    for r in range(1, north):
        pl.semaphore_signal(barrier, inc=1, device_id={"north": lax.rem(me_n + r, north)})

    def x_step(y, carry):
        high, low = split(src[y])
        both = dot(tx[...], jnp.concatenate([high, low], axis=0))
        modes = both[:kept_x] + both[kept_x:]
        at = pl.multiple_of(y * north, north)
        for e in range(each):
            for d in range(deep):
                first = (e * deep + d) * north
                send1[e, d, pl.ds(at, north), :] = modes[first : first + north]
        return carry

    lax.fori_loop(0, ny_part, x_step, 0)
    pl.semaphore_wait(barrier, deep + north - 2)

    copies1 = {}
    for e in range(each):
        for r in range(1, deep):
            to = lax.rem(me_d + r, deep)
            copies1[e, r] = pltpu.make_async_remote_copy(
                src_ref=send1.at[e, to],
                dst_ref=recv1.at[e, me_d],
                send_sem=s1.at[e, r],
                recv_sem=r1.at[e, r],
                device_id={"deep": to},
            )
            copies1[e, r].start()

    def table_step(a, carry):
        table = sin_a[pl.ds(a, 1), :] * cos_b[...] + cos_a[pl.ds(a, 1), :] * sin_b[...]
        high, low = split(table)
        at = pl.multiple_of(a * FINE, FINE)
        t_high[pl.ds(at, FINE), :] = high
        t_low[pl.ds(at, FINE), :] = low
        return carry

    lax.fori_loop(0, sin_a.shape[0], table_step, 0)

    def z_product(values, owner, first):
        high, low = split(values)
        left[:rows, :] = high
        left[rows:, :] = low
        at = pl.multiple_of(owner * nz_part, nz_part)

        def z_step(t, carry):
            cols = pl.ds(pl.multiple_of(t * TILE, TILE), TILE)
            both = dot(left[...], t_high[pl.ds(at, nz_part), cols])
            total = both[:rows] + both[rows:] + dot(left[:rows, :], t_low[pl.ds(at, nz_part), cols])
            if first:
                acc[:, cols] = total
            else:
                acc[:, cols] += total
            return carry

        lax.fori_loop(0, kept_z // TILE, z_step, 0)

    copies2 = {}
    for e in range(each):
        z_product(send1[e, me_d], me_d, True)
        for r in range(1, deep):
            copies1[e, r].wait_recv()
            owner = lax.rem(me_d - r + deep, deep)
            z_product(recv1[e, owner], owner, False)
        for c in range(0, kept_z, TILE):
            part = acc[:, c : c + TILE].reshape(ny_part, north, TILE)
            send2[e, :, :, c : c + TILE] = jnp.swapaxes(part, 0, 1)
        recv2[e, me_n] = send2[e, me_n]
        for r in range(1, north):
            to = lax.rem(me_n + r, north)
            copies2[e, r] = pltpu.make_async_remote_copy(
                src_ref=send2.at[e, to],
                dst_ref=recv2.at[e, me_n],
                send_sem=s2.at[e, r],
                recv_sem=r2.at[e, r],
                device_id={"north": to},
            )
            copies2[e, r].start()

    copies3 = {}
    kept_y = ny_part * north // 2
    share_y = kept_y // deep
    for e in range(each):
        for r in range(1, north):
            copies2[e, r].wait_recv()
        for c in range(0, kept_z, TILE):
            values = recv2[e, :, :, c : c + TILE].reshape(rows, TILE)
            both = dot(ty[...], jnp.concatenate(split(values), axis=0))
            modes = both[:kept_y] + both[kept_y:]
            send3[e, :, :, c : c + TILE] = modes.reshape(deep, share_y, TILE)
        recv3[me_d, e] = send3[e, me_d]
        for r in range(1, deep):
            to = lax.rem(me_d + r, deep)
            copies3[e, r] = pltpu.make_async_remote_copy(
                src_ref=send3.at[e, to],
                dst_ref=recv3.at[me_d, e],
                send_sem=s3.at[e, r],
                recv_sem=r3.at[e, r],
                device_id={"deep": to},
            )
            copies3[e, r].start()

    for copies in (copies1, copies2):
        for copy in copies.values():
            copy.wait_send()
    for copy in copies3.values():
        copy.wait()
    out[...] = recv3[...]


def on_device(source, symbol_x, symbol_y, symbol_z):
    north, deep = lax.axis_size("north"), lax.axis_size("deep")
    nx, ny_part, nz_part = source.shape
    each = nx // 2 // north // deep
    ny, nz = ny_part * north, nz_part * deep
    kept_z, share_y = nz // 2, ny // 2 // deep
    order = np.arange(nx // 2).reshape(north, deep, each).transpose(2, 1, 0).reshape(-1)
    x_high, x_low = left_table(nx)
    tx = stacked(x_high[order], x_low[order])
    ty = stacked(*left_table(ny))
    rows = ny_part * north
    vmem = pl.BlockSpec(memory_space=pltpu.VMEM)
    v = pl.pallas_call(
        functools.partial(kernel, north, deep, each),
        out_shape=jax.ShapeDtypeStruct((deep, each, share_y, kept_z), F32),
        in_specs=[vmem] * 7,
        out_specs=vmem,
        scratch_shapes=[
            pltpu.VMEM((each, deep, rows, nz_part), F32),
            pltpu.VMEM((each, deep, rows, nz_part), F32),
            pltpu.VMEM((each, north, ny_part, kept_z), F32),
            pltpu.VMEM((each, north, ny_part, kept_z), F32),
            pltpu.VMEM((each, deep, share_y, kept_z), F32),
            pltpu.VMEM((deep, each, share_y, kept_z), F32),
            pltpu.VMEM((nz, kept_z), BF16),
            pltpu.VMEM((nz, kept_z), BF16),
            pltpu.VMEM((2 * rows, nz_part), BF16),
            pltpu.VMEM((rows, kept_z), F32),
        ]
        + [pltpu.SemaphoreType.DMA((each, n)) for n in (deep, deep, north, north, deep, deep)],
        compiler_params=pltpu.CompilerParams(
            collective_id=0, has_side_effects=True, vmem_limit_bytes=67043328
        ),
    )(jnp.swapaxes(source, 0, 1), tx, ty, *long_tables(nz))
    v = v.reshape(deep * each, share_y, kept_z)
    part_x = lax.dynamic_slice_in_dim(symbol_x, lax.axis_index("north") * v.shape[0], v.shape[0])
    part_y = lax.dynamic_slice_in_dim(symbol_y, lax.axis_index("deep") * v.shape[1], v.shape[1])
    symbol = part_x[:, None, None] + part_y[None, :, None] + symbol_z[: v.shape[2]][None, None, :]
    return v * lax.rsqrt(symbol)


def solution(mesh):
    in_specs = (P(None, "north", "deep"), P(), P(), P())
    out_specs = P("north", "deep", None)
    return jax.shard_map(
        on_device, mesh=mesh, in_specs=in_specs, out_specs=out_specs, check_vma=False
    )
```

```python
import functools

import jax
import jax.numpy as jnp
import numpy as np
from jax import lax
from jax.experimental import pallas as pl
from jax.experimental.pallas import tpu as pltpu
from jax.sharding import PartitionSpec as P

F32, BF16 = jnp.float32, jnp.bfloat16
FINE = 32
TILE = 256
SUB = 8


def angles(rows, modes, count):
    rank = np.outer(rows, modes) % (2 * count + 2)
    return np.pi / (count + 1) * rank


def split_np(table):
    high = table.astype(np.float32).astype(BF16)
    low = (table - high.astype(np.float64)).astype(np.float32).astype(BF16)
    return high, low


def left_table(count):
    gain = (2.0 / (count + 1)) ** 0.5
    table = np.sin(angles(np.arange(1, count // 2 + 1), np.arange(1, count + 1), count)) * gain
    return split_np(table)


def stacked(high, low):
    return jnp.asarray(np.block([[high, high], [low, np.zeros_like(low)]]))


def long_tables(count):
    modes = np.arange(1, count // 2 + 1)
    gain = (2.0 / (count + 1)) ** 0.5
    coarse = angles(np.arange(0, count, FINE), modes, count)
    step = angles(np.arange(1, FINE + 1), modes, count)
    f32 = lambda v: jnp.asarray(v.astype(np.float32))
    return f32(np.sin(coarse) * gain), f32(np.cos(coarse) * gain), f32(np.sin(step)), f32(np.cos(step))


def split(values):
    high = values.astype(BF16)
    return high, (values - high.astype(F32)).astype(BF16)


def dot(a, b):
    return jnp.dot(a, b, preferred_element_type=F32)


def kernel(
    north, deep, each,
    src, tx, ty, sin_a, cos_a, sin_b, cos_b, symbol_x, symbol_y, symbol_z,
    out,
    turned, send1, recv1, send2, recv2, send3, recv3, t_high, t_low, left, acc,
    s1, r1, s2, r2, s3, r3,
):
    me_n, me_d = lax.axis_index("north"), lax.axis_index("deep")
    nx, ny_part, nz_part = src.shape
    halves = ny_part // SUB
    kept_x = nx // 2
    kept_z = t_high.shape[1]
    rows = SUB * north
    kept_y = ny_part * north // 2
    share_y = kept_y // deep

    barrier = pltpu.get_barrier_semaphore()
    for r in range(1, deep):
        pl.semaphore_signal(barrier, inc=1, device_id={"deep": lax.rem(me_d + r, deep)})
    for r in range(1, north):
        pl.semaphore_signal(barrier, inc=1, device_id={"north": lax.rem(me_n + r, north)})

    def x_product(h):
        for c in range(0, nz_part, TILE):

            def turn(g, carry):
                at = pl.multiple_of(g * 16, 16)
                part = src[pl.ds(at, 16), h * SUB : (h + 1) * SUB, c : c + TILE]
                high, low = split(jnp.swapaxes(part, 0, 1))
                turned[:, pl.ds(at, 16), :] = high
                turned[:, pl.ds(pl.multiple_of(nx + at, 16), 16), :] = low
                return carry

            lax.fori_loop(0, nx // 16, turn, 0)

            def x_step(y, carry):
                both = dot(tx[...], turned[y])
                modes = both[:kept_x] + both[kept_x:]
                at = pl.multiple_of(y * north, north)
                for e in range(each):
                    for d in range(deep):
                        first = (e * deep + d) * north
                        send1[e, h, d, pl.ds(at, north), c : c + TILE] = modes[first : first + north]
                return carry

            lax.fori_loop(0, SUB, x_step, 0)

    copies1 = {}

    def send_modes(e, h):
        for r in range(1, deep):
            to = lax.rem(me_d + r, deep)
            copies1[e, h, r] = pltpu.make_async_remote_copy(
                src_ref=send1.at[e, h, to],
                dst_ref=recv1.at[e, h, me_d],
                send_sem=s1.at[e * halves + h, r],
                recv_sem=r1.at[e * halves + h, r],
                device_id={"deep": to},
            )
            copies1[e, h, r].start()

    for h in range(halves):
        x_product(h)
        if h == 0:
            pl.semaphore_wait(barrier, deep + north - 2)
        send_modes(0, h)
    for e in range(1, each):
        for h in range(halves):
            send_modes(e, h)

    def table_step(a, carry):
        table = sin_a[pl.ds(a, 1), :] * cos_b[...] + cos_a[pl.ds(a, 1), :] * sin_b[...]
        high, low = split(table)
        at = pl.multiple_of(a * FINE, FINE)
        t_high[pl.ds(at, FINE), :] = high
        t_low[pl.ds(at, FINE), :] = low
        return carry

    lax.fori_loop(0, sin_a.shape[0], table_step, 0)

    def inverse_roots():
        row = lax.broadcasted_iota(jnp.int32, (share_y, TILE), 0)
        part_y = jnp.zeros((share_y, TILE), F32)
        for j in range(share_y):
            part_y = jnp.where(row == j, symbol_y[me_d * share_y + j], part_y)
        for d in range(deep):
            for e in range(each):
                part_x = symbol_x[me_n * deep * each + d * each + e]
                for c in range(0, kept_z, TILE):
                    out[d, e, :, c : c + TILE] = lax.rsqrt(part_x + part_y + symbol_z[:, c : c + TILE])

    inverse_roots()

    def z_product(values, owner, first):
        high, low = split(values)
        left[:rows, :] = high
        left[rows:, :] = low
        at = pl.multiple_of(owner * nz_part, nz_part)

        def z_step(t, carry):
            cols = pl.ds(pl.multiple_of(t * TILE, TILE), TILE)
            both = dot(left[...], t_high[pl.ds(at, nz_part), cols])
            total = both[:rows] + both[rows:] + dot(left[:rows, :], t_low[pl.ds(at, nz_part), cols])
            if first:
                acc[:, cols] = total
            else:
                acc[:, cols] += total
            return carry

        lax.fori_loop(0, kept_z // TILE, z_step, 0)

    copies2 = {}
    for e in range(each):
        for h in range(halves):
            z_product(send1[e, h, me_d], me_d, True)
            for r in range(1, deep):
                copies1[e, h, r].wait_recv()
                owner = lax.rem(me_d - r + deep, deep)
                z_product(recv1[e, h, owner], owner, False)
            for c in range(0, kept_z, TILE):
                part = acc[:, c : c + TILE].reshape(SUB, north, TILE)
                send2[e, h, :, :, c : c + TILE] = jnp.swapaxes(part, 0, 1)
            recv2[e, h, me_n] = send2[e, h, me_n]
            for r in range(1, north):
                to = lax.rem(me_n + r, north)
                copies2[e, h, r] = pltpu.make_async_remote_copy(
                    src_ref=send2.at[e, h, to],
                    dst_ref=recv2.at[e, h, me_n],
                    send_sem=s2.at[e * halves + h, r],
                    recv_sem=r2.at[e * halves + h, r],
                    device_id={"north": to},
                )
                copies2[e, h, r].start()

    copies3 = {}
    for e in range(each):
        for h in range(halves):
            for r in range(1, north):
                copies2[e, h, r].wait_recv()
        for c in range(0, kept_z, TILE):
            values = recv2[e, :, :, :, c : c + TILE].reshape(ny_part * north, TILE)
            both = dot(ty[...], jnp.concatenate(split(values), axis=0))
            modes = both[:kept_y] + both[kept_y:]
            send3[e, :, :, c : c + TILE] = modes.reshape(deep, share_y, TILE)
        recv3[me_d, e] = send3[e, me_d]
        for r in range(1, deep):
            to = lax.rem(me_d + r, deep)
            copies3[e, r] = pltpu.make_async_remote_copy(
                src_ref=send3.at[e, to],
                dst_ref=recv3.at[me_d, e],
                send_sem=s3.at[e, r],
                recv_sem=r3.at[e, r],
                device_id={"deep": to},
            )
            copies3[e, r].start()

    for copies in (copies1, copies2):
        for copy in copies.values():
            copy.wait_send()
    for copy in copies3.values():
        copy.wait()
    out[...] = out[...] * recv3[...]


def on_device(source, symbol_x, symbol_y, symbol_z):
    north, deep = lax.axis_size("north"), lax.axis_size("deep")
    nx, ny_part, nz_part = source.shape
    each, halves = nx // 2 // north // deep, ny_part // SUB
    ny, nz = ny_part * north, nz_part * deep
    kept_z, share_y = nz // 2, ny // 2 // deep
    order = np.arange(nx // 2).reshape(north, deep, each).transpose(2, 1, 0).reshape(-1)
    x_high, x_low = left_table(nx)
    tx = stacked(x_high[order], x_low[order])
    order = np.arange(ny).reshape(north, halves, SUB).transpose(1, 0, 2).reshape(-1)
    y_high, y_low = left_table(ny)
    ty = stacked(y_high[:, order], y_low[:, order])
    rows = SUB * north
    vmem = pl.BlockSpec(memory_space=pltpu.VMEM)
    smem = pl.BlockSpec(memory_space=pltpu.SMEM)
    chunks = each * halves
    v = pl.pallas_call(
        functools.partial(kernel, north, deep, each),
        out_shape=jax.ShapeDtypeStruct((deep, each, share_y, kept_z), F32),
        in_specs=[vmem] * 7 + [smem] * 2 + [vmem],
        out_specs=vmem,
        scratch_shapes=[
            pltpu.VMEM((SUB, 2 * nx, TILE), BF16),
            pltpu.VMEM((each, halves, deep, rows, nz_part), F32),
            pltpu.VMEM((each, halves, deep, rows, nz_part), F32),
            pltpu.VMEM((each, halves, north, SUB, kept_z), F32),
            pltpu.VMEM((each, halves, north, SUB, kept_z), F32),
            pltpu.VMEM((each, deep, share_y, kept_z), F32),
            pltpu.VMEM((deep, each, share_y, kept_z), F32),
            pltpu.VMEM((nz, kept_z), BF16),
            pltpu.VMEM((nz, kept_z), BF16),
            pltpu.VMEM((2 * rows, nz_part), BF16),
            pltpu.VMEM((rows, kept_z), F32),
        ]
        + [
            pltpu.SemaphoreType.DMA((sets, peers))
            for sets, peers in ((chunks, deep), (chunks, north), (each, deep))
            for _ in range(2)
        ],
        compiler_params=pltpu.CompilerParams(
            collective_id=0, has_side_effects=True, vmem_limit_bytes=67043328
        ),
    )(source, tx, ty, *long_tables(nz), symbol_x, symbol_y, symbol_z[None, :])
    return v.reshape(deep * each, share_y, kept_z)


def solution(mesh):
    in_specs = (P(None, "north", "deep"), P(), P(), P())
    out_specs = P("north", "deep", None)
    return jax.shard_map(
        on_device, mesh=mesh, in_specs=in_specs, out_specs=out_specs, check_vma=False
    )
```

```python
import functools

import jax
import jax.numpy as jnp
import numpy as np
from jax import lax
from jax.experimental import pallas as pl
from jax.experimental.pallas import tpu as pltpu
from jax.sharding import PartitionSpec as P

F32, BF16 = jnp.float32, jnp.bfloat16
FINE = 32
TILE = 256
SUB = 8


def angles(rows, modes, count):
    rank = np.outer(rows, modes) % (2 * count + 2)
    return np.pi / (count + 1) * rank


def split_np(table):
    high = table.astype(np.float32).astype(BF16)
    low = (table - high.astype(np.float64)).astype(np.float32).astype(BF16)
    return high, low


def left_table(count):
    gain = (2.0 / (count + 1)) ** 0.5
    table = np.sin(angles(np.arange(1, count // 2 + 1), np.arange(1, count + 1), count)) * gain
    return split_np(table)


def stacked(high, low):
    return jnp.asarray(np.block([[high, high], [low, np.zeros_like(low)]]))


def long_tables(count):
    modes = np.arange(1, count // 2 + 1)
    gain = (2.0 / (count + 1)) ** 0.5
    coarse = angles(np.arange(0, count, FINE), modes, count)
    step = angles(np.arange(1, FINE + 1), modes, count)
    f32 = lambda v: jnp.asarray(v.astype(np.float32))
    return f32(np.sin(coarse) * gain), f32(np.cos(coarse) * gain), f32(np.sin(step)), f32(np.cos(step))


def split(values):
    high = values.astype(BF16)
    return high, (values - high.astype(F32)).astype(BF16)


def dot(a, b):
    return jnp.dot(a, b, preferred_element_type=F32)


def kernel(
    north, deep, each,
    source, tx, ty, sin_a, cos_a, sin_b, cos_b, symbol_x, symbol_y, symbol_z,
    out,
    src, turned, send1, recv1, send2, recv2, send3, recv3, t_high, t_low, left, acc,
    s1, r1, s2, r2, s3, r3, loaded,
):
    me_n, me_d = lax.axis_index("north"), lax.axis_index("deep")
    nx, ny_part, nz_part = src.shape
    halves = ny_part // SUB
    kept_x = nx // 2
    kept_z = t_high.shape[1]
    rows = SUB * north
    kept_y = ny_part * north // 2
    share_y = kept_y // deep

    loads = []
    for h in range(halves):
        planes = (slice(None), pl.ds(h * SUB, SUB))
        loads.append(pltpu.make_async_copy(source.at[planes], src.at[planes], loaded.at[h]))
        loads[h].start()

    barrier = pltpu.get_barrier_semaphore()
    for r in range(1, deep):
        pl.semaphore_signal(barrier, inc=1, device_id={"deep": lax.rem(me_d + r, deep)})
    for r in range(1, north):
        pl.semaphore_signal(barrier, inc=1, device_id={"north": lax.rem(me_n + r, north)})

    def x_product(h):
        for c in range(0, nz_part, TILE):

            def turn(g, carry):
                at = pl.multiple_of(g * 16, 16)
                part = src[pl.ds(at, 16), h * SUB : (h + 1) * SUB, c : c + TILE]
                high, low = split(jnp.swapaxes(part, 0, 1))
                turned[:, pl.ds(at, 16), :] = high
                turned[:, pl.ds(pl.multiple_of(nx + at, 16), 16), :] = low
                return carry

            lax.fori_loop(0, nx // 16, turn, 0)

            def x_step(y, carry):
                both = dot(tx[...], turned[y])
                modes = both[:kept_x] + both[kept_x:]
                at = pl.multiple_of(y * north, north)
                for e in range(each):
                    for d in range(deep):
                        first = (e * deep + d) * north
                        send1[e, h, d, pl.ds(at, north), c : c + TILE] = modes[first : first + north]
                return carry

            lax.fori_loop(0, SUB, x_step, 0)

    copies1 = {}

    def send_modes(e, h):
        for r in range(1, deep):
            to = lax.rem(me_d + r, deep)
            copies1[e, h, r] = pltpu.make_async_remote_copy(
                src_ref=send1.at[e, h, to],
                dst_ref=recv1.at[e, h, me_d],
                send_sem=s1.at[e * halves + h, r],
                recv_sem=r1.at[e * halves + h, r],
                device_id={"deep": to},
            )
            copies1[e, h, r].start()

    for h in range(halves):
        loads[h].wait()
        x_product(h)
        if h == 0:
            pl.semaphore_wait(barrier, deep + north - 2)
        send_modes(0, h)
    for e in range(1, each):
        for h in range(halves):
            send_modes(e, h)

    def table_step(a, carry):
        table = sin_a[pl.ds(a, 1), :] * cos_b[...] + cos_a[pl.ds(a, 1), :] * sin_b[...]
        high, low = split(table)
        at = pl.multiple_of(a * FINE, FINE)
        t_high[pl.ds(at, FINE), :] = high
        t_low[pl.ds(at, FINE), :] = low
        return carry

    lax.fori_loop(0, sin_a.shape[0], table_step, 0)

    def inverse_roots():
        row = lax.broadcasted_iota(jnp.int32, (share_y, TILE), 0)
        part_y = jnp.zeros((share_y, TILE), F32)
        for j in range(share_y):
            part_y = jnp.where(row == j, symbol_y[me_d * share_y + j], part_y)
        for d in range(deep):
            for e in range(each):
                part_x = symbol_x[me_n * deep * each + d * each + e]
                for c in range(0, kept_z, TILE):
                    out[d, e, :, c : c + TILE] = lax.rsqrt(part_x + part_y + symbol_z[:, c : c + TILE])

    inverse_roots()

    def z_product(values, owner, first):
        high, low = split(values)
        left[:rows, :] = high
        left[rows:, :] = low
        at = pl.multiple_of(owner * nz_part, nz_part)

        def z_step(t, carry):
            cols = pl.ds(pl.multiple_of(t * TILE, TILE), TILE)
            both = dot(left[...], t_high[pl.ds(at, nz_part), cols])
            total = both[:rows] + both[rows:] + dot(left[:rows, :], t_low[pl.ds(at, nz_part), cols])
            if first:
                acc[:, cols] = total
            else:
                acc[:, cols] += total
            return carry

        lax.fori_loop(0, kept_z // TILE, z_step, 0)

    copies2 = {}
    for e in range(each):
        for h in range(halves):
            z_product(send1[e, h, me_d], me_d, True)
            for r in range(1, deep):
                copies1[e, h, r].wait_recv()
                owner = lax.rem(me_d - r + deep, deep)
                z_product(recv1[e, h, owner], owner, False)
            for c in range(0, kept_z, TILE):
                part = acc[:, c : c + TILE].reshape(SUB, north, TILE)
                send2[e, h, :, :, c : c + TILE] = jnp.swapaxes(part, 0, 1)
            recv2[e, h, me_n] = send2[e, h, me_n]
            for r in range(1, north):
                to = lax.rem(me_n + r, north)
                copies2[e, h, r] = pltpu.make_async_remote_copy(
                    src_ref=send2.at[e, h, to],
                    dst_ref=recv2.at[e, h, me_n],
                    send_sem=s2.at[e * halves + h, r],
                    recv_sem=r2.at[e * halves + h, r],
                    device_id={"north": to},
                )
                copies2[e, h, r].start()

    copies3 = {}
    for e in range(each):
        for h in range(halves):
            for r in range(1, north):
                copies2[e, h, r].wait_recv()
        for c in range(0, kept_z, TILE):
            values = recv2[e, :, :, :, c : c + TILE].reshape(ny_part * north, TILE)
            both = dot(ty[...], jnp.concatenate(split(values), axis=0))
            modes = both[:kept_y] + both[kept_y:]
            send3[e, :, :, c : c + TILE] = modes.reshape(deep, share_y, TILE)
        recv3[me_d, e] = send3[e, me_d]
        for r in range(1, deep):
            to = lax.rem(me_d + r, deep)
            copies3[e, r] = pltpu.make_async_remote_copy(
                src_ref=send3.at[e, to],
                dst_ref=recv3.at[me_d, e],
                send_sem=s3.at[e, r],
                recv_sem=r3.at[e, r],
                device_id={"deep": to},
            )
            copies3[e, r].start()

    for copies in (copies1, copies2):
        for copy in copies.values():
            copy.wait_send()
    for copy in copies3.values():
        copy.wait()
    out[...] = out[...] * recv3[...]


def on_device(source, symbol_x, symbol_y, symbol_z):
    north, deep = lax.axis_size("north"), lax.axis_size("deep")
    nx, ny_part, nz_part = source.shape
    each, halves = nx // 2 // north // deep, ny_part // SUB
    ny, nz = ny_part * north, nz_part * deep
    kept_z, share_y = nz // 2, ny // 2 // deep
    order = np.arange(nx // 2).reshape(north, deep, each).transpose(2, 1, 0).reshape(-1)
    x_high, x_low = left_table(nx)
    tx = stacked(x_high[order], x_low[order])
    order = np.arange(ny).reshape(north, halves, SUB).transpose(1, 0, 2).reshape(-1)
    y_high, y_low = left_table(ny)
    ty = stacked(y_high[:, order], y_low[:, order])
    rows = SUB * north
    vmem = pl.BlockSpec(memory_space=pltpu.VMEM)
    smem = pl.BlockSpec(memory_space=pltpu.SMEM)
    chunks = each * halves
    v = pl.pallas_call(
        functools.partial(kernel, north, deep, each),
        out_shape=jax.ShapeDtypeStruct((deep, each, share_y, kept_z), F32),
        in_specs=[pl.BlockSpec(memory_space=pl.ANY)] + [vmem] * 6 + [smem] * 2 + [vmem],
        out_specs=vmem,
        scratch_shapes=[
            pltpu.VMEM(source.shape, F32),
            pltpu.VMEM((SUB, 2 * nx, TILE), BF16),
            pltpu.VMEM((each, halves, deep, rows, nz_part), F32),
            pltpu.VMEM((each, halves, deep, rows, nz_part), F32),
            pltpu.VMEM((each, halves, north, SUB, kept_z), F32),
            pltpu.VMEM((each, halves, north, SUB, kept_z), F32),
            pltpu.VMEM((each, deep, share_y, kept_z), F32),
            pltpu.VMEM((deep, each, share_y, kept_z), F32),
            pltpu.VMEM((nz, kept_z), BF16),
            pltpu.VMEM((nz, kept_z), BF16),
            pltpu.VMEM((2 * rows, nz_part), BF16),
            pltpu.VMEM((rows, kept_z), F32),
        ]
        + [
            pltpu.SemaphoreType.DMA((sets, peers))
            for sets, peers in ((chunks, deep), (chunks, north), (each, deep))
            for _ in range(2)
        ]
        + [pltpu.SemaphoreType.DMA((halves,))],
        compiler_params=pltpu.CompilerParams(
            collective_id=0, has_side_effects=True, vmem_limit_bytes=67043328
        ),
    )(source, tx, ty, *long_tables(nz), symbol_x, symbol_y, symbol_z[None, :])
    return v.reshape(deep * each, share_y, kept_z)


def solution(mesh):
    in_specs = (P(None, "north", "deep"), P(), P(), P())
    out_specs = P("north", "deep", None)
    return jax.shard_map(
        on_device, mesh=mesh, in_specs=in_specs, out_specs=out_specs, check_vma=False
    )
```
